32 devices in a mesh: freq: 4 (over y, core), stn: 8 (over z, x).
Axes of the slice: x: 2, y: 2, z: 4, core: 2. Of those that a mesh axis runs over, the one named last changes fastest.
Arguments:
- samples: bfloat16 [4, 256, 24, 2, 128], P('freq', 'stn'), may hold values from -8 to 8, as said below
- window: float32 [128], replicated, may hold values from 0.1 to 1
- group_of_device: int32 [8], replicated, may hold values from 0 to 7, each once
- owner_map: int32 [8, 8], replicated, may hold values from 0 to 7, as said below
Outputs:
- owned: bfloat16 [2, 32, 8, 8, 1024], P(None, None, 'stn', 'freq')
The draws below stay inside these ranges and needn't reach their ends.
Inputs may be any that keep to these rules, and one draw needn't show every extreme that they name: `samples`: samples are finite and bounded. Every row and every column of owner_map names each stn index exactly once.
All inputs are finite; a program needn't handle non-finite values.
Results may differ from the reference program's by a relative error of at most 0.0065.
Values may be sent and summed in bfloat16 or wider, within the bound.
No kernel may reach another device: no remote copies, remote signals or barrier semaphores. Data moves between devices by JAX's collectives and lax.ppermute only.
A program may use at most 64 MiB of HBM per device.

```python
import math
import jax
import jax.numpy as jnp
from jax import lax

FFT_LEN = 128
AVG = 16
SPEC = 24
GRP_IN = 32
CH_OUT = 8
GROUPS = 8
BANDS = 4
INPUTS = 256
CHANNELS = 32


def draw_samples(key, part):
    sky_sources = 32
    keys = jax.random.split(key, 3)
    shape = (BANDS, INPUTS, SPEC, 2, FFT_LEN)
    gains = jax.random.normal(keys[1], (INPUTS, sky_sources), jnp.float32)
    signals = jax.random.normal(keys[2], (BANDS, sky_sources, SPEC, 2, FFT_LEN), jnp.float32)
    common = jnp.einsum('ik,bktrn->bitrn', gains, signals) / math.sqrt(sky_sources)
    noise = jax.random.normal(keys[0], shape, jnp.float32)
    total = 0.55 * noise + common
    return jnp.clip(total, -8.0, 8.0).astype(jnp.bfloat16)


def draw_owner_map(key, part):
    keys = jax.random.split(key, 3)
    row_shift = jax.random.permutation(keys[0], GROUPS)
    col_shift = jax.random.permutation(keys[1], GROUPS)
    labels = jax.random.permutation(keys[2], GROUPS)
    return labels[(row_shift[:, None] + col_shift[None, :]) % GROUPS].astype(jnp.int32)


def setup_inputs(seed: int = 0) -> dict:
    key_of = jax.random.split(jax.random.key(seed), 5)
    return {
        "samples": draw_samples(jax.random.fold_in(key_of[4], 71), 0),
        "window": jnp.clip(jnp.exp(jax.random.uniform(key_of[1], (FFT_LEN,), jnp.float32, math.log(0.1), math.log(1.0))), 0.1, 1.0),
        "group_of_device": jax.random.permutation(key_of[2], GROUPS).astype(jnp.int32),
        "owner_map": draw_owner_map(jax.random.fold_in(key_of[4], 71), 0),
    }


def channel_matrix(window):
    length = window.shape[0]
    index = jnp.arange(length, dtype=jnp.int32)
    product = index[:, None] * index[None, :] % length
    theta = product.astype(jnp.float32) * (2.0 * math.pi / length)
    weights = window[:, None] / math.sqrt(length)
    cosine = weights * jnp.cos(theta)
    sine = weights * jnp.sin(theta)
    upper = jnp.concatenate([cosine, -sine], axis=1)
    lower = jnp.concatenate([sine, cosine], axis=1)
    return jnp.concatenate([upper, lower], axis=0)

def split_matrix(matrix):
    high = matrix.astype(jnp.bfloat16)
    low = (matrix - high.astype(jnp.float32)).astype(jnp.bfloat16)
    return (high, low)

def channelize(block, high, low):
    rows = block.shape[0]
    flat = block.reshape(rows * SPEC, 2 * FFT_LEN)
    spectra = jnp.dot(flat, high, preferred_element_type=jnp.float32) + jnp.dot(flat, low, preferred_element_type=jnp.float32)
    spectra = spectra.astype(jnp.bfloat16).reshape(rows, SPEC, 2, CH_OUT, AVG)
    return spectra.transpose(3, 0, 2, 1, 4).reshape(CH_OUT, rows, 2 * SPEC * AVG)

def reference(samples, window, group_of_device, owner_map):
    high, low = split_matrix(channel_matrix(window))
    order = jnp.arange(GROUPS, dtype=jnp.int32)
    dev_of_group = jnp.zeros((GROUPS,), jnp.int32).at[group_of_device].set(order)
    grouped = samples.reshape(BANDS, GROUPS, GRP_IN, SPEC, 2, FFT_LEN)
    grouped = jnp.take(grouped, dev_of_group, axis=1).reshape(BANDS, INPUTS, SPEC, 2, FFT_LEN)
    column_for = jnp.zeros((GROUPS, GROUPS), jnp.int32).at[order[:, None], owner_map].set(jnp.broadcast_to(order[None, :], (GROUPS, GROUPS)))

    def one_band(band):
        spectra = channelize(band, high, low).astype(jnp.float32)
        half = spectra.shape[2] // 2
        swapped = jnp.concatenate([spectra[..., half:], -spectra[..., :half]], axis=-1)
        stacked = jnp.stack([spectra, swapped])
        vis = jnp.einsum('pcak,cbk->pcab', stacked, spectra)
        vis = (vis * (1.0 / (AVG * SPEC))).astype(jnp.bfloat16)
        vis = vis.reshape(2, CH_OUT, GROUPS, GRP_IN, GROUPS, GRP_IN).transpose(0, 1, 2, 4, 3, 5)
        vis = vis.reshape(2, CH_OUT, GROUPS, GROUPS, GRP_IN * GRP_IN)
        picked = jnp.take_along_axis(vis, column_for[None, None, :, :, None], axis=3)
        return picked.transpose(0, 1, 3, 2, 4)
    result = lax.map(one_band, grouped)
    result = result.transpose(1, 0, 2, 3, 4, 5)
    return result.reshape(2, CHANNELS, GROUPS, GROUPS, GRP_IN * GRP_IN)
```

```python
import functools
import math

import jax
import jax.numpy as jnp
import numpy as np
from jax import lax
from jax.experimental import pallas as pl
from jax.experimental.pallas import tpu as pltpu
from jax.sharding import PartitionSpec as P

FFT_LEN = 128
AVG = 16
SPEC = 24
CH_OUT = 8
LANES = 128


def trig_table():
    index = np.arange(FFT_LEN)
    theta = (index[:, None] * index[None, :] % FFT_LEN) * (2.0 * math.pi / FFT_LEN)
    table = np.concatenate([np.cos(theta), np.sin(theta)], axis=0) / math.sqrt(FFT_LEN)
    return table.astype(np.float32)


def barrel(values, lane_chunk):
    n = len(values)
    step = 1
    while step < n:
        bit = (lane_chunk // step) % 2 == 1
        values = [jnp.where(bit, values[(i - step) % n], values[i]) for i in range(n)]
        step *= 2
    return values


def channelize_kernel(rows, x_ref, window_ref, table_ref, out_ref, cos_ref, sin_ref):
    matrix = table_ref[...] * window_ref[...]
    high = matrix.astype(jnp.bfloat16)
    low = (matrix - high.astype(jnp.float32)).astype(jnp.bfloat16)
    both = jnp.concatenate([high, low], axis=1)
    x = x_ref[...]
    y = lax.dot_general(
        jnp.concatenate([x, x], axis=1),
        both,
        (((1,), (1,)), ((), ())),
        preferred_element_type=jnp.float32,
    )
    cos_ref[...] = y[:, :FFT_LEN]
    sin_ref[...] = y[:, FFT_LEN:]
    chunk = lax.broadcasted_iota(jnp.int32, (rows, LANES), 1) // AVG
    tiles = SPEC // CH_OUT
    for tile in range(tiles):
        real, imag = [], []
        for m in range(CH_OUT):
            t = tile * CH_OUT + m
            even = pl.ds(2 * t, rows, stride=2 * SPEC)
            odd = pl.ds(2 * t + 1, rows, stride=2 * SPEC)
            re = cos_ref[even, :] + sin_ref[odd, :]
            im = cos_ref[odd, :] - sin_ref[even, :]
            if m:
                re = pltpu.roll(re, m * AVG, 1)
                im = pltpu.roll(im, m * AVG, 1)
            real.append(re)
            imag.append(im)
        for p, part in enumerate((real, imag)):
            part = barrel([part[-i % CH_OUT] for i in range(CH_OUT)], chunk)
            at = (p * tiles + tile) * LANES
            for k in range(CH_OUT):
                out_ref[k, :, at : at + LANES] = part[k].astype(jnp.bfloat16)


def channelize(block, window):
    rows = block.shape[0]
    flat = block.reshape(rows * SPEC * 2, FFT_LEN)
    return pl.pallas_call(
        functools.partial(channelize_kernel, rows),
        out_shape=jax.ShapeDtypeStruct((CH_OUT, rows, 2 * SPEC * AVG), jnp.bfloat16),
        scratch_shapes=[pltpu.VMEM((rows * SPEC * 2, FFT_LEN), jnp.float32)] * 2,
    )(flat, window[None, :], jnp.asarray(trig_table()))


def correlate_kernel(groups, rows, god_ref, om_ref, x_ref, out_ref, *vis_refs):
    x = x_ref[...]
    half = x.shape[1] // 2
    swapped = jnp.concatenate([x[:, half:], -x[:, :half]], axis=1)
    per_tile = LANES // rows
    per_row = groups // out_ref.shape[0]
    chunk = lax.broadcasted_iota(jnp.int32, (rows // per_tile, LANES), 1) // rows
    for p, left in enumerate((x, swapped)):
        vis = lax.dot_general(
            left, x, (((1,), (1,)), ((), ())), preferred_element_type=jnp.float32
        )
        vis = vis * (1.0 / (AVG * SPEC))
        for h, ref in enumerate(vis_refs):
            ref[p] = vis[:, h * LANES : (h + 1) * LANES]
    for s in range(groups):
        g1 = god_ref[s]
        f, r = g1 // per_row, g1 % per_row
        for h, ref in enumerate(vis_refs):
            owners = [om_ref[g1, god_ref[h * per_tile + c]] for c in range(per_tile)]
            for p in range(2):
                parts = []
                for m in range(per_tile):
                    u = ref[p, pl.ds(s * rows + m, rows // per_tile, stride=per_tile), :]
                    parts.append(pltpu.roll(u, m * rows, 1) if m else u)
                parts = barrel([parts[-i % per_tile] for i in range(per_tile)], chunk)
                for c in range(per_tile):
                    block = parts[c]
                    if c:
                        block = pltpu.roll(block, LANES - c * rows, 1)
                    out_ref[f, owners[c], p, r] = block.astype(jnp.bfloat16)


def correlate(turned, group_of_device, owner_map, bands):
    groups = group_of_device.shape[0]
    rows = turned.shape[0] // groups
    per_tile = LANES // rows
    vmem = pl.BlockSpec(memory_space=pltpu.VMEM)
    smem = pl.BlockSpec(memory_space=pltpu.SMEM)
    return pl.pallas_call(
        functools.partial(correlate_kernel, groups, rows),
        in_specs=[smem, smem, vmem],
        out_specs=vmem,
        out_shape=jax.ShapeDtypeStruct(
            (bands, groups, 2, groups // bands, rows // per_tile, LANES), jnp.bfloat16
        ),
        scratch_shapes=[pltpu.VMEM((2, groups * rows, LANES), jnp.float32)]
        * (groups // per_tile),
    )(group_of_device, owner_map, turned)


def with_swapped(spectra):
    half = spectra.shape[2] // 2
    return jnp.stack(
        [spectra, jnp.concatenate([spectra[..., half:], -spectra[..., :half]], axis=-1)]
    )


def correlate_wide(stacked, remote):
    block = jnp.einsum("pcak,cbk->pcab", stacked, remote, preferred_element_type=jnp.float32)
    return (block * (1.0 / (AVG * SPEC))).astype(jnp.bfloat16)


def wide_plan(local, group_of_device, owner_map, here, groups):
    order = jnp.arange(groups, dtype=jnp.int32)
    device_of_group = jnp.zeros((groups,), jnp.int32).at[group_of_device].set(order)
    rows_in = local.shape[1]
    spread = groups // CH_OUT
    quarter = here % spread
    copies = jnp.repeat(local, spread, axis=0)
    turned = lax.all_to_all(copies, "stn", split_axis=0, concat_axis=1, tiled=True)
    span = CH_OUT * rows_in
    mine = lax.dynamic_slice_in_dim(turned, quarter * span, span, 1)
    block = correlate_wide(with_swapped(mine), turned)
    column_for = (
        jnp.zeros((groups, groups), jnp.int32)
        .at[order[:, None], owner_map]
        .set(jnp.broadcast_to(order[None, :], (groups, groups)))
    )
    row_source = quarter * CH_OUT + jnp.arange(CH_OUT, dtype=jnp.int32)
    row_group = group_of_device[row_source]
    column_device = device_of_group[column_for[row_group]]
    vis = block.reshape(2, CH_OUT, rows_in, groups, rows_in).transpose(0, 1, 3, 2, 4)
    picked = jnp.take_along_axis(vis, column_device[None, :, :, None, None], axis=2)
    outgoing = picked.reshape(2, CH_OUT, groups, rows_in * rows_in)
    received = lax.all_to_all(outgoing, "stn", split_axis=2, concat_axis=2, tiled=True)
    arranged = received.reshape(2, CH_OUT, CH_OUT, spread, rows_in * rows_in).transpose(
        0, 2, 3, 1, 4
    )
    arranged = arranged.reshape(2, CH_OUT, groups, rows_in * rows_in)
    by_group = jnp.take(arranged, device_of_group, axis=2)
    regrouped = lax.all_to_all(by_group, "freq", split_axis=2, concat_axis=1, tiled=True)
    return regrouped[:, :, None]


def shards(samples, window, group_of_device, owner_map):
    groups = lax.axis_size("stn")
    bands = lax.axis_size("freq")
    here = lax.axis_index("stn")
    local = channelize(samples[0], window)
    if groups != CH_OUT:
        return wide_plan(local, group_of_device, owner_map, here, groups)
    rows = local.shape[1]
    turned = lax.all_to_all(local, "stn", split_axis=0, concat_axis=0, tiled=True)
    blocks = correlate(
        turned.reshape(groups * rows, local.shape[2]), group_of_device, owner_map, bands
    )
    shape = blocks.shape
    blocks = blocks.reshape((bands * groups,) + shape[2:])
    owned = lax.all_to_all(blocks, ("freq", "stn"), split_axis=0, concat_axis=0, tiled=True)
    owned = owned.transpose(1, 0, 2, 3, 4)
    return owned.reshape(2, bands * CH_OUT, 1, groups // bands, rows * rows)


def solution(mesh):
    return jax.shard_map(
        shards,
        mesh=mesh,
        in_specs=(P("freq", "stn", None, None, None), P(), P(), P()),
        out_specs=P(None, None, "stn", "freq", None),
        check_vma=False,
    )
```

```python
import functools
import math

import jax
import jax.numpy as jnp
import numpy as np
from jax import lax
from jax.experimental import pallas as pl
from jax.experimental.pallas import tpu as pltpu
from jax.sharding import PartitionSpec as P

FFT_LEN = 128
AVG = 16
SPEC = 24
CH_OUT = 8
LANES = 128


def trig_table():
    index = np.arange(FFT_LEN)
    theta = (index[:, None] * index[None, :] % FFT_LEN) * (2.0 * math.pi / FFT_LEN)
    table = np.concatenate([np.cos(theta), np.sin(theta)], axis=0) / math.sqrt(FFT_LEN)
    return table.astype(np.float32)


def barrel(values, lane_chunk):
    n = len(values)
    step = 1
    while step < n:
        bit = (lane_chunk // step) % 2 == 1
        values = [jnp.where(bit, values[(i - step) % n], values[i]) for i in range(n)]
        step *= 2
    return values


def channelize_kernel(rows, here_ref, x_ref, window_ref, table_ref, *refs):
    *out_refs, by_channel, cos_ref, sin_ref = refs
    matrix = table_ref[...] * window_ref[...]
    high = matrix.astype(jnp.bfloat16)
    low = (matrix - high.astype(jnp.float32)).astype(jnp.bfloat16)
    both = jnp.concatenate([high, low], axis=1)
    x = x_ref[...]
    y = lax.dot_general(
        jnp.concatenate([x, x], axis=1),
        both,
        (((1,), (1,)), ((), ())),
        preferred_element_type=jnp.float32,
    )
    cos_ref[...] = y[:, :FFT_LEN]
    sin_ref[...] = y[:, FFT_LEN:]
    chunk = lax.broadcasted_iota(jnp.int32, (rows, LANES), 1) // AVG
    tiles = SPEC // CH_OUT
    for tile in range(tiles):
        real, imag = [], []
        for m in range(CH_OUT):
            t = tile * CH_OUT + m
            even = pl.ds(2 * t, rows, stride=2 * SPEC)
            odd = pl.ds(2 * t + 1, rows, stride=2 * SPEC)
            re = cos_ref[even, :] + sin_ref[odd, :]
            im = cos_ref[odd, :] - sin_ref[even, :]
            if m:
                re = pltpu.roll(re, m * AVG, 1)
                im = pltpu.roll(im, m * AVG, 1)
            real.append(re)
            imag.append(im)
        for p, part in enumerate((real, imag)):
            part = barrel([part[-i % CH_OUT] for i in range(CH_OUT)], chunk)
            at = (p * tiles + tile) * LANES
            for k in range(CH_OUT):
                by_channel[k, :, at : at + LANES] = part[k].astype(jnp.bfloat16)
    for d, out_ref in enumerate(out_refs):
        out_ref[...] = by_channel[here_ref[0] ^ d]


def channelize(block, window, start):
    rows = block.shape[0]
    shape = (rows, 2 * SPEC * AVG)
    vmem = pl.BlockSpec(memory_space=pltpu.VMEM)
    flat = block.reshape(rows * SPEC * 2, FFT_LEN)
    return pl.pallas_call(
        functools.partial(channelize_kernel, rows),
        in_specs=[pl.BlockSpec(memory_space=pltpu.SMEM), vmem, vmem, vmem],
        out_specs=[vmem] * CH_OUT,
        out_shape=[jax.ShapeDtypeStruct(shape, jnp.bfloat16)] * CH_OUT,
        scratch_shapes=[pltpu.VMEM((CH_OUT,) + shape, jnp.bfloat16)]
        + [pltpu.VMEM((rows * SPEC * 2, FFT_LEN), jnp.float32)] * 2,
    )(jnp.full((1,), start, jnp.int32), flat, window[None, :], jnp.asarray(trig_table()))


def correlate_kernel(groups, rows, here_ref, god_ref, om_ref, *refs):
    x_refs, out_ref, vis_refs = refs[:groups], refs[groups], refs[groups + 1 :]
    x = jnp.concatenate([ref[...] for ref in x_refs], axis=0)
    group = [god_ref[here_ref[0] ^ d] for d in range(groups)]
    half = x.shape[1] // 2
    swapped = jnp.concatenate([x[:, half:], -x[:, :half]], axis=1)
    per_tile = LANES // rows
    per_row = groups // out_ref.shape[0]
    chunk = lax.broadcasted_iota(jnp.int32, (rows // per_tile, LANES), 1) // rows
    for p, left in enumerate((x, swapped)):
        vis = lax.dot_general(
            left, x, (((1,), (1,)), ((), ())), preferred_element_type=jnp.float32
        )
        vis = vis * (1.0 / (AVG * SPEC))
        for h, ref in enumerate(vis_refs):
            ref[p] = vis[:, h * LANES : (h + 1) * LANES]
    for s in range(groups):
        g1 = group[s]
        f, r = g1 // per_row, g1 % per_row
        for h, ref in enumerate(vis_refs):
            owners = [om_ref[g1, group[h * per_tile + c]] for c in range(per_tile)]
            for p in range(2):
                parts = []
                for m in range(per_tile):
                    u = ref[p, pl.ds(s * rows + m, rows // per_tile, stride=per_tile), :]
                    parts.append(pltpu.roll(u, m * rows, 1) if m else u)
                parts = barrel([parts[-i % per_tile] for i in range(per_tile)], chunk)
                for c in range(per_tile):
                    block = parts[c]
                    if c:
                        block = pltpu.roll(block, LANES - c * rows, 1)
                    out_ref[f, owners[c], p, r] = block.astype(jnp.bfloat16)


def correlate(turned, here, group_of_device, owner_map, bands):
    groups = group_of_device.shape[0]
    rows = turned[0].shape[0]
    per_tile = LANES // rows
    vmem = pl.BlockSpec(memory_space=pltpu.VMEM)
    smem = pl.BlockSpec(memory_space=pltpu.SMEM)
    return pl.pallas_call(
        functools.partial(correlate_kernel, groups, rows),
        in_specs=[smem, smem, smem] + [vmem] * groups,
        out_specs=vmem,
        out_shape=jax.ShapeDtypeStruct(
            (bands, groups, 2, groups // bands, rows // per_tile, LANES), jnp.bfloat16
        ),
        scratch_shapes=[pltpu.VMEM((2, groups * rows, LANES), jnp.float32)]
        * (groups // per_tile),
    )(jnp.full((1,), here, jnp.int32), group_of_device, owner_map, *turned)


def with_swapped(spectra):
    half = spectra.shape[2] // 2
    return jnp.stack(
        [spectra, jnp.concatenate([spectra[..., half:], -spectra[..., :half]], axis=-1)]
    )


def correlate_wide(stacked, remote):
    block = jnp.einsum("pcak,cbk->pcab", stacked, remote, preferred_element_type=jnp.float32)
    return (block * (1.0 / (AVG * SPEC))).astype(jnp.bfloat16)


def wide_plan(local, group_of_device, owner_map, here, groups):
    order = jnp.arange(groups, dtype=jnp.int32)
    device_of_group = jnp.zeros((groups,), jnp.int32).at[group_of_device].set(order)
    rows_in = local.shape[1]
    spread = groups // CH_OUT
    quarter = here % spread
    copies = jnp.repeat(local, spread, axis=0)
    turned = lax.all_to_all(copies, "stn", split_axis=0, concat_axis=1, tiled=True)
    span = CH_OUT * rows_in
    mine = lax.dynamic_slice_in_dim(turned, quarter * span, span, 1)
    block = correlate_wide(with_swapped(mine), turned)
    column_for = (
        jnp.zeros((groups, groups), jnp.int32)
        .at[order[:, None], owner_map]
        .set(jnp.broadcast_to(order[None, :], (groups, groups)))
    )
    row_source = quarter * CH_OUT + jnp.arange(CH_OUT, dtype=jnp.int32)
    row_group = group_of_device[row_source]
    column_device = device_of_group[column_for[row_group]]
    vis = block.reshape(2, CH_OUT, rows_in, groups, rows_in).transpose(0, 1, 3, 2, 4)
    picked = jnp.take_along_axis(vis, column_device[None, :, :, None, None], axis=2)
    outgoing = picked.reshape(2, CH_OUT, groups, rows_in * rows_in)
    received = lax.all_to_all(outgoing, "stn", split_axis=2, concat_axis=2, tiled=True)
    arranged = received.reshape(2, CH_OUT, CH_OUT, spread, rows_in * rows_in).transpose(
        0, 2, 3, 1, 4
    )
    arranged = arranged.reshape(2, CH_OUT, groups, rows_in * rows_in)
    by_group = jnp.take(arranged, device_of_group, axis=2)
    regrouped = lax.all_to_all(by_group, "freq", split_axis=2, concat_axis=1, tiled=True)
    return regrouped[:, :, None]


def shards(samples, window, group_of_device, owner_map):
    groups = lax.axis_size("stn")
    bands = lax.axis_size("freq")
    here = lax.axis_index("stn")
    if groups != CH_OUT:
        local = jnp.stack(channelize(samples[0], window, 0))
        return wide_plan(local, group_of_device, owner_map, here, groups)
    local = channelize(samples[0], window, here)
    rows = local[0].shape[0]
    turned = [local[0]] + [
        lax.ppermute(local[d], "stn", [(s, s ^ d) for s in range(groups)])
        for d in range(1, groups)
    ]
    blocks = correlate(turned, here, group_of_device, owner_map, bands)
    shape = blocks.shape
    blocks = blocks.reshape((bands * groups,) + shape[2:])
    owned = lax.all_to_all(blocks, ("freq", "stn"), split_axis=0, concat_axis=0, tiled=True)
    owned = owned.transpose(1, 0, 2, 3, 4)
    return owned.reshape(2, bands * CH_OUT, 1, groups // bands, rows * rows)


def solution(mesh):
    return jax.shard_map(
        shards,
        mesh=mesh,
        in_specs=(P("freq", "stn", None, None, None), P(), P(), P()),
        out_specs=P(None, None, "stn", "freq", None),
        check_vma=False,
    )
```

```python
import functools
import math

import jax
import jax.numpy as jnp
import numpy as np
from jax import lax
from jax.experimental import pallas as pl
from jax.experimental.pallas import tpu as pltpu
from jax.sharding import PartitionSpec as P

FFT_LEN = 128
AVG = 16
SPEC = 24
CH_OUT = 8
LANES = 128


def trig_table():
    index = np.arange(FFT_LEN)
    theta = (index[:, None] * index[None, :] % FFT_LEN) * (2.0 * math.pi / FFT_LEN)
    table = np.concatenate([np.cos(theta), np.sin(theta)], axis=0) / math.sqrt(FFT_LEN)
    return table.astype(np.float32)


def barrel(values, lane_chunk):
    n = len(values)
    step = 1
    while step < n:
        bit = (lane_chunk // step) % 2 == 1
        values = [jnp.where(bit, values[(i - step) % n], values[i]) for i in range(n)]
        step *= 2
    return values


def channelize_kernel(rows, here_ref, x_ref, window_ref, table_ref, *refs):
    *out_refs, by_channel, cos_ref, sin_ref = refs
    matrix = table_ref[...] * window_ref[...]
    high = matrix.astype(jnp.bfloat16)
    low = (matrix - high.astype(jnp.float32)).astype(jnp.bfloat16)
    both = jnp.concatenate([high, low], axis=1)
    x = x_ref[...]
    y = lax.dot_general(
        jnp.concatenate([x, x], axis=1),
        both,
        (((1,), (1,)), ((), ())),
        preferred_element_type=jnp.float32,
    )
    cos_ref[...] = y[:, :FFT_LEN]
    sin_ref[...] = y[:, FFT_LEN:]
    chunk = lax.broadcasted_iota(jnp.int32, (rows, LANES), 1) // AVG
    tiles = SPEC // CH_OUT
    for tile in range(tiles):
        real, imag = [], []
        for m in range(CH_OUT):
            t = tile * CH_OUT + m
            even = pl.ds(2 * t, rows, stride=2 * SPEC)
            odd = pl.ds(2 * t + 1, rows, stride=2 * SPEC)
            re = cos_ref[even, :] + sin_ref[odd, :]
            im = cos_ref[odd, :] - sin_ref[even, :]
            if m:
                re = pltpu.roll(re, m * AVG, 1)
                im = pltpu.roll(im, m * AVG, 1)
            real.append(re)
            imag.append(im)
        for p, part in enumerate((real, imag)):
            part = barrel([part[-i % CH_OUT] for i in range(CH_OUT)], chunk)
            at = (p * tiles + tile) * LANES
            for k in range(CH_OUT):
                by_channel[k, :, at : at + LANES] = part[k].astype(jnp.bfloat16)
    for d, out_ref in enumerate(out_refs):
        out_ref[...] = by_channel[here_ref[0] ^ d]


def channelize(block, window, start):
    rows = block.shape[0]
    shape = (rows, 2 * SPEC * AVG)
    vmem = pl.BlockSpec(memory_space=pltpu.VMEM)
    flat = block.reshape(rows * SPEC * 2, FFT_LEN)
    return pl.pallas_call(
        functools.partial(channelize_kernel, rows),
        in_specs=[pl.BlockSpec(memory_space=pltpu.SMEM), vmem, vmem, vmem],
        out_specs=[vmem] * CH_OUT,
        out_shape=[pltpu.VMEM(shape, jnp.bfloat16)] * CH_OUT,
        scratch_shapes=[pltpu.VMEM((CH_OUT,) + shape, jnp.bfloat16)]
        + [pltpu.VMEM((rows * SPEC * 2, FFT_LEN), jnp.float32)] * 2,
    )(jnp.full((1,), start, jnp.int32), flat, window[None, :], jnp.asarray(trig_table()))


def correlate_kernel(groups, rows, here_ref, god_ref, om_ref, *refs):
    x_refs, out_ref, vis_refs = refs[:groups], refs[groups], refs[groups + 1 :]
    x = jnp.concatenate([ref[...] for ref in x_refs], axis=0)
    group = [god_ref[here_ref[0] ^ d] for d in range(groups)]
    half = x.shape[1] // 2
    swapped = jnp.concatenate([x[:, half:], -x[:, :half]], axis=1)
    per_tile = LANES // rows
    per_row = groups // out_ref.shape[0]
    chunk = lax.broadcasted_iota(jnp.int32, (rows // per_tile, LANES), 1) // rows
    for p, left in enumerate((x, swapped)):
        vis = lax.dot_general(
            left, x, (((1,), (1,)), ((), ())), preferred_element_type=jnp.float32
        )
        vis = vis * (1.0 / (AVG * SPEC))
        for h, ref in enumerate(vis_refs):
            ref[p] = vis[:, h * LANES : (h + 1) * LANES]
    for s in range(groups):
        g1 = group[s]
        f, r = g1 // per_row, g1 % per_row
        for h, ref in enumerate(vis_refs):
            owners = [om_ref[g1, group[h * per_tile + c]] for c in range(per_tile)]
            for p in range(2):
                parts = []
                for m in range(per_tile):
                    u = ref[p, pl.ds(s * rows + m, rows // per_tile, stride=per_tile), :]
                    parts.append(pltpu.roll(u, m * rows, 1) if m else u)
                parts = barrel([parts[-i % per_tile] for i in range(per_tile)], chunk)
                for c in range(per_tile):
                    block = parts[c]
                    if c:
                        block = pltpu.roll(block, LANES - c * rows, 1)
                    out_ref[f, owners[c], p, r] = block.astype(jnp.bfloat16)


def correlate(turned, here, group_of_device, owner_map, bands):
    groups = group_of_device.shape[0]
    rows = turned[0].shape[0]
    per_tile = LANES // rows
    turned = [pltpu.with_memory_space_constraint(x, pltpu.VMEM) for x in turned]
    vmem = pl.BlockSpec(memory_space=pltpu.VMEM)
    smem = pl.BlockSpec(memory_space=pltpu.SMEM)
    return pl.pallas_call(
        functools.partial(correlate_kernel, groups, rows),
        in_specs=[smem, smem, smem] + [vmem] * groups,
        out_specs=vmem,
        out_shape=pltpu.VMEM(
            (bands, groups, 2, groups // bands, rows // per_tile, LANES), jnp.bfloat16
        ),
        scratch_shapes=[pltpu.VMEM((2, groups * rows, LANES), jnp.float32)]
        * (groups // per_tile),
    )(jnp.full((1,), here, jnp.int32), group_of_device, owner_map, *turned)


def with_swapped(spectra):
    half = spectra.shape[2] // 2
    return jnp.stack(
        [spectra, jnp.concatenate([spectra[..., half:], -spectra[..., :half]], axis=-1)]
    )


def correlate_wide(stacked, remote):
    block = jnp.einsum("pcak,cbk->pcab", stacked, remote, preferred_element_type=jnp.float32)
    return (block * (1.0 / (AVG * SPEC))).astype(jnp.bfloat16)


def wide_plan(local, group_of_device, owner_map, here, groups):
    order = jnp.arange(groups, dtype=jnp.int32)
    device_of_group = jnp.zeros((groups,), jnp.int32).at[group_of_device].set(order)
    rows_in = local.shape[1]
    spread = groups // CH_OUT
    quarter = here % spread
    copies = jnp.repeat(local, spread, axis=0)
    turned = lax.all_to_all(copies, "stn", split_axis=0, concat_axis=1, tiled=True)
    span = CH_OUT * rows_in
    mine = lax.dynamic_slice_in_dim(turned, quarter * span, span, 1)
    block = correlate_wide(with_swapped(mine), turned)
    column_for = (
        jnp.zeros((groups, groups), jnp.int32)
        .at[order[:, None], owner_map]
        .set(jnp.broadcast_to(order[None, :], (groups, groups)))
    )
    row_source = quarter * CH_OUT + jnp.arange(CH_OUT, dtype=jnp.int32)
    row_group = group_of_device[row_source]
    column_device = device_of_group[column_for[row_group]]
    vis = block.reshape(2, CH_OUT, rows_in, groups, rows_in).transpose(0, 1, 3, 2, 4)
    picked = jnp.take_along_axis(vis, column_device[None, :, :, None, None], axis=2)
    outgoing = picked.reshape(2, CH_OUT, groups, rows_in * rows_in)
    received = lax.all_to_all(outgoing, "stn", split_axis=2, concat_axis=2, tiled=True)
    arranged = received.reshape(2, CH_OUT, CH_OUT, spread, rows_in * rows_in).transpose(
        0, 2, 3, 1, 4
    )
    arranged = arranged.reshape(2, CH_OUT, groups, rows_in * rows_in)
    by_group = jnp.take(arranged, device_of_group, axis=2)
    regrouped = lax.all_to_all(by_group, "freq", split_axis=2, concat_axis=1, tiled=True)
    return regrouped[:, :, None]


def shards(samples, window, group_of_device, owner_map):
    groups = lax.axis_size("stn")
    bands = lax.axis_size("freq")
    here = lax.axis_index("stn")
    if groups != CH_OUT:
        local = jnp.stack(channelize(samples[0], window, 0))
        return wide_plan(local, group_of_device, owner_map, here, groups)
    local = channelize(samples[0], window, here)
    rows = local[0].shape[0]
    turned = {0: local[0]}
    for d in range(groups - 1, 0, -1):
        turned[d] = lax.ppermute(local[d], "stn", [(s, s ^ d) for s in range(groups)])
    turned = [turned[d] for d in range(groups)]
    blocks = correlate(turned, here, group_of_device, owner_map, bands)
    shape = blocks.shape
    blocks = blocks.reshape((bands * groups,) + shape[2:])
    owned = lax.all_to_all(blocks, ("freq", "stn"), split_axis=0, concat_axis=0, tiled=True)
    owned = owned.transpose(1, 0, 2, 3, 4)
    return owned.reshape(2, bands * CH_OUT, 1, groups // bands, rows * rows)


def solution(mesh):
    return jax.shard_map(
        shards,
        mesh=mesh,
        in_specs=(P("freq", "stn", None, None, None), P(), P(), P()),
        out_specs=P(None, None, "stn", "freq", None),
        check_vma=False,
    )
```

```python
import functools
import math

import jax
import jax.numpy as jnp
import numpy as np
from jax import lax
from jax.experimental import pallas as pl
from jax.experimental.pallas import tpu as pltpu
from jax.sharding import PartitionSpec as P


FFT_LEN = 128
AVG = 16
SPEC = 24
CH_OUT = 8
LANES = 128


def trig_table():
    index = np.arange(FFT_LEN)
    theta = (index[:, None] * index[None, :] % FFT_LEN) * (2.0 * math.pi / FFT_LEN)
    table = np.concatenate([np.cos(theta), np.sin(theta)], axis=0) / math.sqrt(FFT_LEN)
    return table.astype(np.float32)


def barrel(values, lane_chunk):
    n = len(values)
    step = 1
    while step < n:
        bit = (lane_chunk // step) % 2 == 1
        values = [jnp.where(bit, values[(i - step) % n], values[i]) for i in range(n)]
        step *= 2
    return values


def channelize_kernel(rows, here_ref, x_ref, window_ref, table_ref, *refs):
    *out_refs, by_channel, cos_ref, sin_ref = refs
    matrix = table_ref[...] * window_ref[...]
    high = matrix.astype(jnp.bfloat16)
    low = (matrix - high.astype(jnp.float32)).astype(jnp.bfloat16)
    both = jnp.concatenate([high, low], axis=1)
    x = x_ref[...]
    y = lax.dot_general(
        jnp.concatenate([x, x], axis=1),
        both,
        (((1,), (1,)), ((), ())),
        preferred_element_type=jnp.float32,
    )
    cos_ref[...] = y[:, :FFT_LEN]
    sin_ref[...] = y[:, FFT_LEN:]
    chunk = lax.broadcasted_iota(jnp.int32, (rows, LANES), 1) // AVG
    tiles = SPEC // CH_OUT
    for tile in range(tiles):
        real, imag = [], []
        for m in range(CH_OUT):
            t = tile * CH_OUT + m
            even = pl.ds(2 * t, rows, stride=2 * SPEC)
            odd = pl.ds(2 * t + 1, rows, stride=2 * SPEC)
            re = cos_ref[even, :] + sin_ref[odd, :]
            im = cos_ref[odd, :] - sin_ref[even, :]
            if m:
                re = pltpu.roll(re, m * AVG, 1)
                im = pltpu.roll(im, m * AVG, 1)
            real.append(re)
            imag.append(im)
        for p, part in enumerate((real, imag)):
            part = barrel([part[-i % CH_OUT] for i in range(CH_OUT)], chunk)
            at = (p * tiles + tile) * LANES
            for k in range(CH_OUT):
                by_channel[k, :, at : at + LANES] = part[k].astype(jnp.bfloat16)
    for d, out_ref in enumerate(out_refs):
        out_ref[...] = by_channel[here_ref[0] ^ d]


def channelize(block, window, start):
    rows = block.shape[0]
    shape = (rows, 2 * SPEC * AVG)
    vmem = pl.BlockSpec(memory_space=pltpu.VMEM)
    flat = block.reshape(rows * SPEC * 2, FFT_LEN)
    return pl.pallas_call(
        functools.partial(channelize_kernel, rows),
        in_specs=[pl.BlockSpec(memory_space=pltpu.SMEM), vmem, vmem, vmem],
        out_specs=[vmem] * CH_OUT,
        out_shape=[pltpu.VMEM(shape, jnp.bfloat16)] * CH_OUT,
        scratch_shapes=[pltpu.VMEM((CH_OUT,) + shape, jnp.bfloat16)]
        + [pltpu.VMEM((rows * SPEC * 2, FFT_LEN), jnp.float32)] * 2,
    )(jnp.full((1,), start, jnp.int32), flat, window[None, :], jnp.asarray(trig_table()))


def correlate_kernel(groups, rows, here_ref, god_ref, om_ref, *refs):
    x_refs, out_ref, vis_refs = refs[:groups], refs[groups], refs[groups + 1 :]
    x = jnp.concatenate([ref[...] for ref in x_refs], axis=0)
    group = [god_ref[here_ref[0] ^ d] for d in range(groups)]
    half = x.shape[1] // 2
    swapped = jnp.concatenate([x[:, half:], -x[:, :half]], axis=1)
    per_tile = LANES // rows
    per_row = groups // out_ref.shape[0]
    chunk = lax.broadcasted_iota(jnp.int32, (rows // per_tile, LANES), 1) // rows
    for p, left in enumerate((x, swapped)):
        vis = lax.dot_general(
            left, x, (((1,), (1,)), ((), ())), preferred_element_type=jnp.float32
        )
        vis = vis * (1.0 / (AVG * SPEC))
        for h, ref in enumerate(vis_refs):
            ref[p] = vis[:, h * LANES : (h + 1) * LANES]
    for s in range(groups):
        g1 = group[s]
        f, r = g1 // per_row, g1 % per_row
        for h, ref in enumerate(vis_refs):
            owners = [om_ref[g1, group[h * per_tile + c]] for c in range(per_tile)]
            for p in range(2):
                parts = []
                for m in range(per_tile):
                    u = ref[p, pl.ds(s * rows + m, rows // per_tile, stride=per_tile), :]
                    parts.append(pltpu.roll(u, m * rows, 1) if m else u)
                parts = barrel([parts[-i % per_tile] for i in range(per_tile)], chunk)
                for c in range(per_tile):
                    block = parts[c]
                    if c:
                        block = pltpu.roll(block, LANES - c * rows, 1)
                    out_ref[f, owners[c], p, r] = block.astype(jnp.bfloat16)


def correlate(turned, here, group_of_device, owner_map, bands):
    groups = group_of_device.shape[0]
    rows = turned[0].shape[0]
    per_tile = LANES // rows
    turned = [pltpu.with_memory_space_constraint(x, pltpu.VMEM) for x in turned]
    vmem = pl.BlockSpec(memory_space=pltpu.VMEM)
    smem = pl.BlockSpec(memory_space=pltpu.SMEM)
    return pl.pallas_call(
        functools.partial(correlate_kernel, groups, rows),
        in_specs=[smem, smem, smem] + [vmem] * groups,
        out_specs=vmem,
        out_shape=pltpu.VMEM(
            (bands, groups, 2, groups // bands, rows // per_tile, LANES), jnp.bfloat16
        ),
        scratch_shapes=[pltpu.VMEM((2, groups * rows, LANES), jnp.float32)]
        * (groups // per_tile),
    )(jnp.full((1,), here, jnp.int32), group_of_device, owner_map, *turned)


def interleave_kernel(in_ref, out_ref):
    chunks = in_ref.shape[3]
    for p in range(2):
        part = in_ref[:, p].astype(jnp.float32)
        for a in range(chunks):
            at = slice(a * LANES, (a + 1) * LANES)
            out_ref[p, :, :, at] = part[:, :, a, :].astype(jnp.bfloat16)


def interleave(blocks):
    n, _, per_row, chunks, _ = blocks.shape
    vmem = pl.BlockSpec(memory_space=pltpu.VMEM)
    return pl.pallas_call(
        interleave_kernel,
        in_specs=[vmem],
        out_specs=vmem,
        out_shape=jax.ShapeDtypeStruct((2, n, per_row, chunks * LANES), jnp.bfloat16),
    )(pltpu.with_memory_space_constraint(blocks, pltpu.VMEM))


def with_swapped(spectra):
    half = spectra.shape[2] // 2
    return jnp.stack(
        [spectra, jnp.concatenate([spectra[..., half:], -spectra[..., :half]], axis=-1)]
    )


def correlate_wide(stacked, remote):
    block = jnp.einsum("pcak,cbk->pcab", stacked, remote, preferred_element_type=jnp.float32)
    return (block * (1.0 / (AVG * SPEC))).astype(jnp.bfloat16)


def wide_plan(local, group_of_device, owner_map, here, groups):
    order = jnp.arange(groups, dtype=jnp.int32)
    device_of_group = jnp.zeros((groups,), jnp.int32).at[group_of_device].set(order)
    rows_in = local.shape[1]
    spread = groups // CH_OUT
    quarter = here % spread
    copies = jnp.repeat(local, spread, axis=0)
    turned = lax.all_to_all(copies, "stn", split_axis=0, concat_axis=1, tiled=True)
    span = CH_OUT * rows_in
    mine = lax.dynamic_slice_in_dim(turned, quarter * span, span, 1)
    block = correlate_wide(with_swapped(mine), turned)
    column_for = (
        jnp.zeros((groups, groups), jnp.int32)
        .at[order[:, None], owner_map]
        .set(jnp.broadcast_to(order[None, :], (groups, groups)))
    )
    row_source = quarter * CH_OUT + jnp.arange(CH_OUT, dtype=jnp.int32)
    row_group = group_of_device[row_source]
    column_device = device_of_group[column_for[row_group]]
    vis = block.reshape(2, CH_OUT, rows_in, groups, rows_in).transpose(0, 1, 3, 2, 4)
    picked = jnp.take_along_axis(vis, column_device[None, :, :, None, None], axis=2)
    outgoing = picked.reshape(2, CH_OUT, groups, rows_in * rows_in)
    received = lax.all_to_all(outgoing, "stn", split_axis=2, concat_axis=2, tiled=True)
    arranged = received.reshape(2, CH_OUT, CH_OUT, spread, rows_in * rows_in).transpose(
        0, 2, 3, 1, 4
    )
    arranged = arranged.reshape(2, CH_OUT, groups, rows_in * rows_in)
    by_group = jnp.take(arranged, device_of_group, axis=2)
    regrouped = lax.all_to_all(by_group, "freq", split_axis=2, concat_axis=1, tiled=True)
    return regrouped[:, :, None]


def shards(samples, window, group_of_device, owner_map):
    groups = lax.axis_size("stn")
    bands = lax.axis_size("freq")
    here = lax.axis_index("stn")
    if groups != CH_OUT:
        local = jnp.stack(channelize(samples[0], window, 0))
        return wide_plan(local, group_of_device, owner_map, here, groups)
    local = channelize(samples[0], window, here)
    rows = local[0].shape[0]
    turned = {0: local[0]}
    for d in range(1, groups):
        turned[d] = lax.ppermute(local[d], "stn", [(s, s ^ d) for s in range(groups)])
    turned = [turned[d] for d in range(groups)]
    blocks = correlate(turned, here, group_of_device, owner_map, bands)
    shape = blocks.shape
    blocks = blocks.reshape((bands * groups,) + shape[2:])
    owned = lax.all_to_all(blocks, ("freq", "stn"), split_axis=0, concat_axis=0, tiled=True)
    return interleave(owned).reshape(2, bands * CH_OUT, 1, groups // bands, rows * rows)


def solution(mesh):
    return jax.shard_map(
        shards,
        mesh=mesh,
        in_specs=(P("freq", "stn", None, None, None), P(), P(), P()),
        out_specs=P(None, None, "stn", "freq", None),
        check_vma=False,
    )
```
